32 devices in a mesh: parts: 2 (over x), shard: 16 (over z, y, core).
Axes of the slice: x: 2, y: 2, z: 4, core: 2. Of those that a mesh axis runs over, the one named last changes fastest.
Arguments:
- queries: bfloat16 [256, 32, 128], P(('parts', 'shard')), parts along dimension 0, may hold values from -6 to 6
- doc_tokens: bfloat16 [256, 128, 128], P(('parts', 'shard')), parts along dimension 0, may hold values from -0.5 to 0.5
- doc_lens: int32 [256], P(('parts', 'shard')), parts along dimension 0, may hold values from 1 to 128
- candidates: int32 [256, 128], P(('parts', 'shard')), parts along dimension 0, may hold values from 0 to 127
Outputs:
- scores: float32 [256, 128], P(('parts', 'shard')), parts along dimension 0
The draws below stay inside these ranges and needn't reach their ends.
There are 2 independent parts, one for each index of `parts`. The reference program is written for one: setup_inputs(seed, part) draws one part's arguments, and reference() takes and returns one part's arrays. A program takes and returns all parts, laid end to end along the dimension named above; each array names one. Nothing has to cross between parts.
Inputs may be any that keep to these rules, and one draw needn't show every extreme that they name: `doc_lens`: every document has at least one live row. `candidates`: ids of documents of the same part.
All inputs are finite; a program needn't handle non-finite values.
Results may differ from the reference program's by a relative error of at most 0.0003.
Values may be sent and summed in bfloat16 or wider, within the bound.
A program may use at most 64 MiB of HBM per device.

```python
import jax
import jax.numpy as jnp
from jax import lax

D = 128
QTOK = 32
BLOCK = 128
CAND = 128
QUERIES = 128
DOCS = 128


def touch_ends(result, key, low, largest):
    place = [jax.random.randint(jax.random.fold_in(key, axis), (), 0, length) for axis, length in enumerate(result.shape)]
    main_axis = result.shape.index(max(result.shape))
    next_to = place[:main_axis] + [(place[main_axis] + 1) % result.shape[main_axis]] + place[main_axis + 1:]
    return result.at[tuple(place)].set(low).at[tuple(next_to)].set(largest)


def steps_of(stream_key, dims, cuts, low, largest):
    def one(dim, blocks):
        draws = jax.random.uniform(jax.random.fold_in(jax.random.fold_in(stream_key, 6), dim), (blocks,), jnp.float32, low / len(cuts), largest / len(cuts))
        return jnp.repeat(jnp.exp(draws), dims[dim] // blocks).reshape((-1,) + (1,) * (len(dims) - dim - 1))

    factor_of = one(*cuts[0])
    for cut in cuts[1:]:
        factor_of = factor_of * one(*cut)
    return factor_of


def bell_draw(key, extent, spread, limit, pieces=(), kind=jnp.bfloat16):
    values = jax.random.normal(key, extent, jnp.float32) * spread
    if len(pieces) > 0:
        values = steps_of(key, extent, pieces, -0.22, 0.18) * values
    return jnp.clip(values, min=-limit, max=limit).astype(kind)


def setup_inputs(seed: int = 0, part: int = 0) -> dict:
    key_list = jax.random.split(jax.random.key(seed), 5)
    part_keys = jax.random.split(jax.random.fold_in(key_list[4], part), 5)
    queries = bell_draw(part_keys[0], (QUERIES, QTOK, D), 1.0, 6.0, ((0, 16),))
    doc_tokens = bell_draw(part_keys[1], (DOCS, BLOCK, D), D ** -0.5, 0.5, ((0, 16),))
    doc_lens = touch_ends(jax.random.randint(part_keys[2], (DOCS,), 1, BLOCK + 1), jax.random.fold_in(part_keys[2], 1), 1, BLOCK).astype(jnp.int32)
    candidates = touch_ends(jax.random.randint(part_keys[3], (QUERIES, CAND), 0, DOCS), jax.random.fold_in(part_keys[3], 1), 0, DOCS - 1).astype(jnp.int32)
    return dict(queries=queries, doc_tokens=doc_tokens, doc_lens=doc_lens, candidates=candidates)


def reference(queries, doc_tokens, doc_lens, candidates):
    rows = jnp.arange(doc_tokens.shape[1], dtype=jnp.int32)

    def one_query(item):
        query, picked = item
        blocks = doc_tokens[picked].astype(jnp.float32)
        live = rows[None, :] < doc_lens[picked][:, None]
        sim = jnp.einsum("id,cjd->cij", query.astype(jnp.float32), blocks)
        sim = jnp.where(live[:, None, :], sim, -1e30)
        return jnp.mean(jnp.max(sim, axis=2), axis=1)

    return lax.map(one_query, (queries, candidates))
```

```python
import functools

import jax
import jax.numpy as jnp
from jax import lax
from jax.experimental import pallas as pl
from jax.experimental.pallas import tpu as pltpu
from jax.sharding import PartitionSpec as P

LANES = 128
MESH = pl.DeviceIdType.MESH


def flip(index, mask):
    out = index
    bit = 1
    while bit <= mask:
        if mask & bit:
            out = out + bit - 2 * bit * ((index // bit) % 2)
        bit *= 2
    return out


def score_kernel(groups, chunks, tokens, lens_ref, q_hbm, d_hbm, table_ref,
                 qbuf, dbuf, best, outgoing, pieces,
                 local_sem, q_send, q_recv, p_send, p_recv, y_send, y_recv, r_send, r_recv, o_send, o_recv):
    part = lax.axis_index("parts")
    me = lax.axis_index("shard")
    k = lax.rem(me, 2)
    b = lax.rem(me // 2, 2)
    g = me // 4

    def at(g_, b_, k_):
        return (part, g_ * 4 + b_ * 2 + k_)

    docs, rows, width = d_hbm.shape
    q_rows = q_hbm.shape[0]
    count = q_rows // tokens
    per_group = 4 * docs
    slot_me = b * 2 + k
    slot_partner = b * 2 + 1 - k
    slot_y = (1 - b) * 2 + k
    slot_yp = (1 - b) * 2 + 1 - k
    step = docs // chunks

    peers = [at(flip(g, j), b, k) for j in range(1, groups)]
    partner = at(g, b, 1 - k)
    across = at(g, 1 - b, k)

    q_in = pltpu.make_async_copy(q_hbm, qbuf.at[g], local_sem.at[0])
    d_in = pltpu.make_async_copy(d_hbm, dbuf.at[slot_me], local_sem.at[1])
    q_in.start()
    d_in.start()

    barrier = pltpu.get_barrier_semaphore()
    for peer in peers + [partner, across]:
        pl.semaphore_signal(barrier, inc=1, device_id=peer, device_id_type=MESH)

    best[...] = jnp.zeros_like(best)
    d_in.wait()
    row_of = lax.broadcasted_iota(jnp.int32, (rows, width), 0)
    for j in range(docs):
        block = dbuf[slot_me, j]
        first = jnp.broadcast_to(block[0:1, :].astype(jnp.float32), (rows, width))
        kept = jnp.where(row_of < lens_ref[j], block.astype(jnp.float32), first)
        dbuf[slot_me, j] = kept.astype(dbuf.dtype)
    q_in.wait()
    pl.semaphore_wait(barrier, len(peers) + 2)

    def remote(src, dst, send, recv, device):
        return pltpu.make_async_remote_copy(src_ref=src, dst_ref=dst, send_sem=send, recv_sem=recv,
                                            device_id=device, device_id_type=MESH)

    def send_queries(j):
        return remote(qbuf.at[g], qbuf.at[g], q_send.at[j - 1], q_recv.at[j - 1], peers[j - 1])

    def doc_chunk(slot, c, send, recv, device):
        ref = dbuf.at[slot, pl.ds(c * step, step)]
        return remote(ref, ref, send.at[c], recv.at[c], device)

    to_partner = remote(dbuf.at[slot_me], dbuf.at[slot_me], p_send, p_recv, partner)
    to_across = [doc_chunk(slot_me, c, y_send, y_recv, across) for c in range(chunks)]
    relays = [doc_chunk(slot_y, c, r_send, r_recv, partner) for c in range(chunks)]
    q_out = [send_queries(j) for j in range(1, groups)]

    to_partner.start()
    if q_out:
        q_out[0].start()
    to_across[0].start()
    for copy in q_out[1:]:
        copy.start()
    for copy in to_across[1:]:
        copy.start()

    base = lax.rem(g, LANES // per_group) * per_group

    def score(j, slot):
        owner = flip(g, j)
        block = dbuf[slot].reshape(docs * rows, width)
        sim = lax.dot_general(block, qbuf[owner], (((1,), (1,)), ((), ())),
                              preferred_element_type=jnp.float32)
        top = jnp.max(sim.reshape(docs, rows, q_rows), axis=1)
        best[j, pl.ds(pl.multiple_of(base + slot * docs, docs), docs), :] = top

    q_of = lax.broadcasted_iota(jnp.int32, (count, q_rows), 1) // tokens
    pick = (q_of == lax.broadcasted_iota(jnp.int32, (count, q_rows), 0)).astype(jnp.float32)
    pick = (pick * (1.0 / tokens)).astype(jnp.bfloat16)

    def reduce_tokens(j):
        rest = best[j]
        total = jnp.zeros((count, LANES), jnp.float32)
        for _ in range(3):
            term = rest.astype(jnp.bfloat16)
            rest = rest - term.astype(jnp.float32)
            total += lax.dot_general(pick, term, (((1,), (1,)), ((), ())),
                                     preferred_element_type=jnp.float32)
        return total

    results = []

    def give(j):
        outgoing[j] = reduce_tokens(j)
        copy = remote(outgoing.at[j], pieces.at[g], o_send.at[j - 1], o_recv.at[j - 1], peers[j - 1])
        copy.start()
        results.append(copy)

    def wait_queries(j):
        q_out[j - 1].wait_recv()

    def pass_on(c):
        to_across[c].wait_recv()
        relays[c].start()

    score(0, slot_me)
    to_partner.wait_recv()
    score(0, slot_partner)
    passed = 0
    last = groups - 1
    for j in range(1, last):
        if passed < chunks:
            pass_on(passed)
            passed += 1
        wait_queries(j)
        score(j, slot_me)
        score(j, slot_partner)
    while passed < chunks:
        pass_on(passed)
        passed += 1
    for j in range(last):
        score(j, slot_y)
    for c in range(chunks):
        relays[c].wait_recv()
    for j in range(1, last):
        score(j, slot_yp)
        give(j)
    wait_queries(last)
    for slot in (slot_me, slot_partner, slot_y, slot_yp):
        score(last, slot)
    give(last)
    score(0, slot_yp)
    pieces[g] = reduce_tokens(0)

    for copy in [to_partner] + to_across + relays + q_out:
        copy.wait_send()
    for copy in results:
        copy.wait_recv()
    wide = LANES // per_group
    for n in range(table_ref.shape[1] // LANES):
        total = pieces[n * wide]
        for s in range(n * wide + 1, (n + 1) * wide):
            total += pieces[s]
        table_ref[:, n * LANES:(n + 1) * LANES] = total
    for copy in results:
        copy.wait_send()


def gather_kernel(table_ref, cand_ref, out_ref):
    cand = cand_ref[...]
    inside = lax.rem(cand, LANES)
    which = cand // LANES
    out = None
    for n in range(table_ref.shape[1] // LANES):
        got = jnp.take_along_axis(table_ref[:, n * LANES:(n + 1) * LANES], inside, axis=1,
                                  mode="promise_in_bounds")
        out = got if out is None else jnp.where(which == n, got, out)
    out_ref[...] = out


def body(shards, queries, doc_tokens, doc_lens, candidates):
    count, tokens, width = queries.shape
    docs, rows, _ = doc_tokens.shape
    groups = shards // 4
    chunks = 4
    q_rows = count * tokens
    dma = pltpu.SemaphoreType.DMA
    others = groups - 1
    table = pl.pallas_call(
        functools.partial(score_kernel, groups, chunks, tokens),
        out_shape=jax.ShapeDtypeStruct((count, shards * docs), jnp.float32),
        in_specs=[
            pl.BlockSpec(memory_space=pltpu.SMEM),
            pl.BlockSpec(memory_space=pl.ANY),
            pl.BlockSpec(memory_space=pl.ANY),
        ],
        out_specs=pl.BlockSpec(memory_space=pltpu.VMEM),
        scratch_shapes=[
            pltpu.VMEM((groups, q_rows, width), queries.dtype),
            pltpu.VMEM((4, docs, rows, width), doc_tokens.dtype),
            pltpu.VMEM((groups, LANES, q_rows), jnp.float32),
            pltpu.VMEM((groups, count, LANES), jnp.float32),
            pltpu.VMEM((groups, count, LANES), jnp.float32),
            dma((2,)),
            dma((others,)), dma((others,)),
            dma, dma,
            dma((chunks,)), dma((chunks,)),
            dma((chunks,)), dma((chunks,)),
            dma((others,)), dma((others,)),
        ],
        compiler_params=pltpu.CompilerParams(collective_id=0, has_side_effects=True),
    )(doc_lens, queries.reshape(q_rows, width), doc_tokens)
    return pl.pallas_call(
        gather_kernel,
        out_shape=jax.ShapeDtypeStruct(candidates.shape, jnp.float32),
    )(table, candidates)


def solution(mesh):
    in_specs = (
        P(("parts", "shard"), None, None),
        P(("parts", "shard"), None, None),
        P(("parts", "shard")),
        P(("parts", "shard"), None),
    )
    out_specs = P(("parts", "shard"), None)
    step = functools.partial(body, mesh.shape["shard"])
    return jax.shard_map(step, mesh=mesh, in_specs=in_specs, out_specs=out_specs, check_vma=False)
```

```python
import functools

import jax
import jax.numpy as jnp
from jax import lax
from jax.experimental import pallas as pl
from jax.experimental.pallas import tpu as pltpu
from jax.sharding import PartitionSpec as P

LANES = 128
MESH = pl.DeviceIdType.MESH


def flip(index, mask):
    out = index
    bit = 1
    while bit <= mask:
        if mask & bit:
            out = out + bit - 2 * bit * ((index // bit) % 2)
        bit *= 2
    return out


def score_kernel(groups, chunks, tokens, lens_ref, q_hbm, d_hbm, table_ref,
                 qbuf, dbuf, best, outgoing, pieces,
                 local_sem, q_send, q_recv, p_send, p_recv, y_send, y_recv, f_send, f_recv, o_send, o_recv):
    part = lax.axis_index("parts")
    me = lax.axis_index("shard")
    k = lax.rem(me, 2)
    b = lax.rem(me // 2, 2)
    g = me // 4

    def at(g_, b_, k_):
        return (part, g_ * 4 + b_ * 2 + k_)

    docs, rows, width = d_hbm.shape
    q_rows = q_hbm.shape[0]
    count = q_rows // tokens
    step = docs // chunks
    slots = {name: b_ * 2 + k_ for name, b_, k_ in
             (("me", b, k), ("partner", b, 1 - k), ("y", 1 - b, k), ("yp", 1 - b, 1 - k))}
    partner = at(g, b, 1 - k)
    across = at(g, 1 - b, k)
    order = [1] + [j for j in range(groups - 1, 1, -1)]

    q_in = pltpu.make_async_copy(q_hbm, qbuf.at[g], local_sem.at[0])
    d_in = pltpu.make_async_copy(d_hbm, dbuf.at[slots["me"]], local_sem.at[1])
    d_in.start()
    q_in.start()

    barrier = pltpu.get_barrier_semaphore()
    takers = [at(flip(g, j), b, k) for j in order]
    for peer in takers + [partner, across]:
        pl.semaphore_signal(barrier, inc=1, device_id=peer, device_id_type=MESH)

    d_in.wait()
    row_of = lax.broadcasted_iota(jnp.int32, (rows, width), 0)
    for j in range(docs):
        block = dbuf[slots["me"], j]
        first = jnp.broadcast_to(block[0:1, :].astype(jnp.float32), (rows, width))
        kept = jnp.where(row_of < lens_ref[j], block.astype(jnp.float32), first)
        dbuf[slots["me"], j] = kept.astype(dbuf.dtype)
    q_in.wait()
    pl.semaphore_wait(barrier, len(takers) + 2)

    def remote(src, dst, send, recv, device):
        return pltpu.make_async_remote_copy(src_ref=src, dst_ref=dst, send_sem=send, recv_sem=recv,
                                            device_id=device, device_id_type=MESH)

    def doc_chunk(name, c, send, recv, device):
        ref = dbuf.at[slots[name], pl.ds(c * step, step)]
        return remote(ref, ref, send.at[c], recv.at[c], device)

    mine = dbuf.at[slots["me"]]
    to_partner = remote(mine, mine, p_send, p_recv, partner)
    to_across = [doc_chunk("me", c, y_send, y_recv, across) for c in range(chunks)]
    relays = [doc_chunk("y", c, f_send, f_recv, partner) for c in range(chunks)]
    q_out = {j: remote(qbuf.at[g], qbuf.at[g], q_send.at[j], q_recv.at[j], peer) for j, peer in zip(order, takers)}

    to_across[0].start()
    for j in order[:2]:
        q_out[j].start()
    to_partner.start()
    for j in order[2:]:
        q_out[j].start()
    for copy in to_across[1:]:
        copy.start()

    have = {name: 0 for name in slots}
    done = {}
    ready = []

    def dot_max(j, name, low, high):
        n = high - low
        u = flip(g, j)
        block = dbuf[slots[name], low:high].reshape(n * rows, width)
        sim = lax.dot_general(block, qbuf[u], (((1,), (1,)), ((), ())), preferred_element_type=jnp.float32)
        best[u * 4 + slots[name], low:high, :] = jnp.max(sim.reshape(n, rows, q_rows), axis=1)

    def catch_up():
        for name in slots:
            for j in ready:
                low = done.get((j, name), 0)
                if low < have[name]:
                    dot_max(j, name, low, have[name])
                    done[j, name] = have[name]

    def arrive(event):
        kind, which = event
        if kind == "q":
            q_out[which].wait_recv()
            ready.append(which)
        elif kind == "p":
            to_partner.wait_recv()
            have["partner"] = docs
        elif kind == "y":
            to_across[which].wait_recv()
            relays[which].start()
            have["y"] += step
        else:
            relays[which].wait_recv()
            have["yp"] += step

    ready.append(0)
    have["me"] = docs
    catch_up()
    arrive(("p", 0))
    catch_up()
    queue = [("q", j) for j in order]
    events = []
    for c in range(chunks):
        if queue:
            events.append(queue.pop(0))
        events.append(("y", c))
        if c > 0:
            events.append(("yp", c - 1))
    for event in queue:
        events.insert(len(events) - 2, event)
    events.append(("yp", chunks - 1))
    for event in events:
        arrive(event)
        catch_up()

    q_of = lax.broadcasted_iota(jnp.int32, (count, q_rows), 1) // tokens
    pick = (q_of == lax.broadcasted_iota(jnp.int32, (count, q_rows), 0)).astype(jnp.float32)
    pick = (pick * (1.0 / tokens)).astype(jnp.bfloat16)
    rest = best[...].reshape(groups * 4 * docs, q_rows)
    total = None
    for _ in range(3):
        term = rest.astype(jnp.bfloat16)
        rest = rest - term.astype(jnp.float32)
        got = lax.dot_general(pick, term, (((1,), (1,)), ((), ())), preferred_element_type=jnp.float32)
        total = got if total is None else total + got
    blocks = total.shape[1] // LANES
    for n in range(blocks):
        outgoing[n] = total[:, n * LANES:(n + 1) * LANES]

    results = [remote(outgoing, pieces.at[g], o_send.at[i], o_recv.at[i], peer) for i, peer in enumerate(takers)]
    for copy in results[::-1]:
        copy.start()
    pieces[g] = outgoing[...]
    for copy in to_across + relays + [to_partner] + list(q_out.values()):
        copy.wait_send()

    per_unit = 4 * docs
    inside = LANES // per_unit
    lane = lax.broadcasted_iota(jnp.int32, (count, LANES), 1) // per_unit
    for copy in results:
        copy.wait_recv()
    for n in range(table_ref.shape[1] // LANES):
        total = None
        for i in range(inside):
            shift = lax.rem(i - lax.rem(g, inside) + inside, inside) * per_unit
            got = pltpu.roll(pieces[n * inside + i, g // inside], shift, 1)
            total = got if total is None else jnp.where(lane == i, got, total)
        table_ref[:, n * LANES:(n + 1) * LANES] = total
    for copy in results:
        copy.wait_send()


def gather_kernel(table_ref, cand_ref, out_ref):
    cand = cand_ref[...]
    inside = lax.rem(cand, LANES)
    which = cand // LANES
    out = None
    for n in range(table_ref.shape[1] // LANES):
        got = jnp.take_along_axis(table_ref[:, n * LANES:(n + 1) * LANES], inside, axis=1,
                                  mode="promise_in_bounds")
        out = got if out is None else jnp.where(which == n, got, out)
    out_ref[...] = out


def body(shards, queries, doc_tokens, doc_lens, candidates):
    count, tokens, width = queries.shape
    docs, rows, _ = doc_tokens.shape
    groups = shards // 4
    chunks = 2
    q_rows = count * tokens
    blocks = groups * 4 * docs // LANES
    dma = pltpu.SemaphoreType.DMA
    table = pl.pallas_call(
        functools.partial(score_kernel, groups, chunks, tokens),
        out_shape=jax.ShapeDtypeStruct((count, shards * docs), jnp.float32),
        in_specs=[
            pl.BlockSpec(memory_space=pltpu.SMEM),
            pl.BlockSpec(memory_space=pl.ANY),
            pl.BlockSpec(memory_space=pl.ANY),
        ],
        out_specs=pl.BlockSpec(memory_space=pltpu.VMEM),
        scratch_shapes=[
            pltpu.VMEM((groups, q_rows, width), queries.dtype),
            pltpu.VMEM((4, docs, rows, width), doc_tokens.dtype),
            pltpu.VMEM((groups * 4, docs, q_rows), jnp.float32),
            pltpu.VMEM((blocks, count, LANES), jnp.float32),
            pltpu.VMEM((groups, blocks, count, LANES), jnp.float32),
            dma((2,)),
            dma((groups,)), dma((groups,)),
            dma, dma,
            dma((chunks,)), dma((chunks,)),
            dma((chunks,)), dma((chunks,)),
            dma((groups,)), dma((groups,)),
        ],
        compiler_params=pltpu.CompilerParams(collective_id=0, has_side_effects=True),
    )(doc_lens, queries.reshape(q_rows, width), doc_tokens)
    return pl.pallas_call(
        gather_kernel,
        out_shape=jax.ShapeDtypeStruct(candidates.shape, jnp.float32),
    )(table, candidates)


def solution(mesh):
    in_specs = (
        P(("parts", "shard"), None, None),
        P(("parts", "shard"), None, None),
        P(("parts", "shard")),
        P(("parts", "shard"), None),
    )
    out_specs = P(("parts", "shard"), None)
    step = functools.partial(body, mesh.shape["shard"])
    return jax.shard_map(step, mesh=mesh, in_specs=in_specs, out_specs=out_specs, check_vma=False)
```
